32 devices in a mesh: row: 8 (over y, x, core), col: 4 (over z).
Axes of the slice: x: 2, y: 2, z: 4, core: 2. Of those that a mesh axis runs over, the one named last changes fastest.
Arguments:
- sources: float32 [8, 4, 512, 512], P('row', 'col'), may hold values from -6 to 6
- leaf_basis: float32 [8, 4, 512, 256], P('row', 'col'), may hold values from -0.25 to 0.25
- transfers: float32 [8, 4, 4, 256, 512], P('row', 'col'), may hold values from -0.25 to 0.25
- out_basis: float32 [8, 4, 512, 256], P('row', 'col'), may hold values from -0.375 to 0.375
Outputs:
- result: float32 [8, 4, 512, 512], P('row', 'col')
The draws below stay inside these ranges and needn't reach their ends.
All inputs are finite; a program needn't handle non-finite values.
Results may differ from the reference program's by a relative error of at most 0.0001.
Values sent between devices are 32-bit elements; how exact they have to be, the bound alone decides.
A program may use at most 64 MiB of HBM per device.

```python
import jax
import jax.numpy as jnp
from jax import lax

LEAF = 512
RANK = 256
RHS = 512
LEVELS = 4
N_ROW = 8
N_COL = 4


def levels(rng, dims, cuts, least, high):
    factor_of = 1.0
    for axis_at, blocks in cuts:
        draws = jax.random.uniform(jax.random.fold_in(jax.random.fold_in(rng, 6), axis_at), (blocks,), jnp.float32, least / len(cuts), high / len(cuts))
        factor_of = factor_of * jnp.repeat(jnp.exp(draws), dims[axis_at] // blocks).reshape((-1,) + (1,) * (len(dims) - 1 - axis_at))
    return factor_of


def gaussian(key, dims, deviation, limit, shards=(), held_as=jnp.bfloat16):
    drawn = deviation * jax.random.normal(key, dims, jnp.float32)
    if shards:
        drawn = drawn * levels(key, dims, shards, -0.22, 0.18)
    return jnp.clip(drawn, -limit, limit).astype(held_as)


def setup_inputs(seed: int = 0) -> dict:
    seeds = jax.random.split(jax.random.key(seed), 5)
    sources = gaussian(seeds[0], (N_ROW, N_COL, LEAF, RHS), 1.0, 6.0, ((0, 8), (1, 4)), jnp.float32)
    leaf_basis = gaussian(seeds[1], (N_ROW, N_COL, LEAF, RANK), LEAF ** -0.5, 0.25, ((0, 8), (1, 4)), jnp.float32)
    transfers = gaussian(seeds[2], (N_ROW, N_COL, LEVELS, RANK, 2 * RANK), (2 * RANK) ** -0.5, 0.25, ((0, 8), (1, 4)), jnp.float32)
    out_basis = gaussian(seeds[3], (N_ROW, N_COL, LEAF, RANK), RANK ** -0.5, 0.375, ((0, 8), (1, 4)), jnp.float32)
    return {"sources": sources, "leaf_basis": leaf_basis, "transfers": transfers, "out_basis": out_basis}


def partner(coeff, axis, bit):
    span = 1 << bit
    shape = coeff.shape
    if axis == 0:
        split = coeff.reshape((shape[0] // (2 * span), 2, span) + shape[1:])
        return jnp.flip(split, 1).reshape(shape)
    split = coeff.reshape((shape[0], shape[1] // (2 * span), 2, span) + shape[2:])
    return jnp.flip(split, 2).reshape(shape)


def reference(sources, leaf_basis, transfers, out_basis):
    high = lax.Precision.HIGHEST
    coeff = jnp.einsum("abmk,abmr->abkr", leaf_basis, sources, precision=high)
    row_bits = N_ROW.bit_length() - 1
    col_bits = N_COL.bit_length() - 1
    for level in range(LEVELS):
        if level % 2 == 0:
            other = partner(coeff, 0, row_bits - 1 - level // 2)
        else:
            other = partner(coeff, 1, col_bits - 1 - level // 2)
        block = transfers[:, :, level]
        coeff = jnp.einsum("abkj,abjr->abkr", block[..., :RANK], coeff, precision=high) + jnp.einsum("abkj,abjr->abkr", block[..., RANK:], other, precision=high)
    return jnp.einsum("abmk,abkr->abmr", out_basis, coeff, precision=high)
```

```python
import functools

import jax
import jax.numpy as jnp
from jax import lax
from jax.experimental import pallas as pl
from jax.experimental.pallas import tpu as pltpu
from jax.sharding import PartitionSpec as P

GROUP = 128
CHUNK = 64


def split(x):
    high = x.astype(jnp.bfloat16)
    return high, (x - high.astype(jnp.float32)).astype(jnp.bfloat16)


def product(left, right_high, right_low, right_dim):
    dims = (((1,), (right_dim,)), ((), ()))
    rows = left.shape[0]
    high, low = split(left)
    both = lax.dot_general(
        jnp.concatenate([high, low], axis=0), right_high, dims, preferred_element_type=jnp.float32
    )
    rest = lax.dot_general(high, right_low, dims, preferred_element_type=jnp.float32)
    return both[:rows] + (both[rows:] + rest)


def order_of(count, levels):
    unit = 8.0 / count
    steps = []
    for at in range(count):
        ready = 3.4 + 2.8 * unit * at
        for level in range(levels):
            steps.append((ready, -level, at, level))
            ready += (3.5 + 1.4 * unit) if level % 2 == 0 else 3.5
    return [(at, level) for _, _, at, level in sorted(steps)]


def partner(level, levels):
    axis = "row" if level % 2 == 0 else "col"
    span = lax.axis_size(axis) >> (1 + level // 2)
    me = lax.axis_index(axis)
    return {axis: me + span - 2 * span * ((me // span) % 2)}


def kernel(
    src, leaf, tra, outb, res,
    src_v, leaf_v, tra_v, outb_v, res_v, coeff, other, t_high, t_low,
    in_sem, tra_sem, out_sem, send_sem, recv_sem,
):
    levels, rank = tra.shape[0], leaf.shape[1]
    rhs = src.shape[1]
    groups, count = rhs // GROUP, rhs // CHUNK
    partners = [partner(level, levels) for level in range(levels)]

    barrier = pltpu.get_barrier_semaphore()
    for who in partners:
        pl.semaphore_signal(barrier, inc=1, device_id=who, device_id_type=pl.DeviceIdType.MESH)

    load_leaf = pltpu.make_async_copy(leaf, leaf_v, in_sem.at[groups])
    load_leaf.start()
    load_src = []
    for g in range(groups):
        cols = pl.ds(g * GROUP, GROUP)
        load_src.append(pltpu.make_async_copy(src.at[:, cols], src_v.at[:, cols], in_sem.at[g]))
        load_src[-1].start()
    load_tra = [pltpu.make_async_copy(tra.at[k], tra_v.at[k], tra_sem.at[k]) for k in range(levels)]
    for copy in load_tra:
        copy.start()
    load_out = pltpu.make_async_copy(outb, outb_v, in_sem.at[groups + 1])
    load_out.start()

    copies = {}

    def send(at, level):
        rows = pl.ds(at * CHUNK, CHUNK)
        copy = pltpu.make_async_remote_copy(
            src_ref=coeff.at[level, rows],
            dst_ref=other.at[level, rows],
            send_sem=send_sem.at[level, at],
            recv_sem=recv_sem.at[level, at],
            device_id=partners[level],
            device_id_type=pl.DeviceIdType.MESH,
        )
        copy.start()
        copies[at, level] = copy

    load_leaf.wait()
    l_high, l_low = split(leaf_v[...])
    for g in range(groups):
        load_src[g].wait()
        turned = src_v[:, g * GROUP:(g + 1) * GROUP].T
        coeff[0, pl.ds(g * GROUP, GROUP), :] = product(turned, l_high, l_low, 0)
        if g == 0:
            pl.semaphore_wait(barrier, levels)
        for at in range(g * GROUP // CHUNK, (g + 1) * GROUP // CHUNK):
            send(at, 0)
    for k in range(levels):
        load_tra[k].wait()
        high, low = split(tra_v[k])
        t_high[k] = high
        t_low[k] = low
    load_out.wait()

    stores = []
    done = set()
    for at, level in order_of(count, levels):
        rows = pl.ds(at * CHUNK, CHUNK)
        own = product(coeff[level, rows, :], t_high[level, :, :rank], t_low[level, :, :rank], 1)
        copies[at, level].wait_recv()
        fresh = own + product(
            other[level, rows, :], t_high[level, :, rank:], t_low[level, :, rank:], 1
        )
        coeff[level + 1, rows, :] = fresh
        if level + 1 < levels:
            send(at, level + 1)
            continue
        done.add(at)
        g = at * CHUNK // GROUP
        if all(m in done for m in range(g * GROUP // CHUNK, (g + 1) * GROUP // CHUNK)):
            cols = pl.ds(g * GROUP, GROUP)
            last_high, last_low = split(coeff[levels, cols, :])
            res_v[:, g * GROUP:(g + 1) * GROUP] = product(outb_v[...], last_high, last_low, 1)
            stores.append(pltpu.make_async_copy(res_v.at[:, cols], res.at[:, cols], out_sem.at[g]))
            stores[-1].start()
    for copy in copies.values():
        copy.wait_send()
    for copy in stores:
        copy.wait()


def body(sources, leaf_basis, transfers, out_basis):
    src, leaf, tra, outb = sources[0, 0], leaf_basis[0, 0], transfers[0, 0], out_basis[0, 0]
    size, rhs = src.shape
    rank = leaf.shape[1]
    levels = tra.shape[0]
    f32 = jnp.float32
    any_space = pl.BlockSpec(memory_space=pl.ANY)
    result = pl.pallas_call(
        kernel,
        out_shape=jax.ShapeDtypeStruct((size, rhs), f32),
        in_specs=[any_space] * 4,
        out_specs=any_space,
        scratch_shapes=[
            pltpu.VMEM((size, rhs), f32),
            pltpu.VMEM((size, rank), f32),
            pltpu.VMEM(tra.shape, f32),
            pltpu.VMEM((size, rank), f32),
            pltpu.VMEM((size, rhs), f32),
            pltpu.VMEM((levels + 1, rhs, rank), f32),
            pltpu.VMEM((levels, rhs, rank), f32),
            pltpu.VMEM(tra.shape, jnp.bfloat16),
            pltpu.VMEM(tra.shape, jnp.bfloat16),
            pltpu.SemaphoreType.DMA((rhs // GROUP + 2,)),
            pltpu.SemaphoreType.DMA((levels,)),
            pltpu.SemaphoreType.DMA((rhs // GROUP,)),
            pltpu.SemaphoreType.DMA((levels, rhs // CHUNK)),
            pltpu.SemaphoreType.DMA((levels, rhs // CHUNK)),
        ],
        compiler_params=pltpu.CompilerParams(collective_id=0, has_side_effects=True),
    )(src, leaf, tra, outb)
    return result[None, None]


def solution(mesh):
    in_specs = (
        P("row", "col", None, None),
        P("row", "col", None, None),
        P("row", "col", None, None, None),
        P("row", "col", None, None),
    )
    out_specs = P("row", "col", None, None)
    return jax.shard_map(body, mesh=mesh, in_specs=in_specs, out_specs=out_specs, check_vma=False)
```

```python
import jax
import jax.numpy as jnp
from jax import lax
from jax.experimental import pallas as pl
from jax.experimental.pallas import tpu as pltpu
from jax.sharding import PartitionSpec as P

GROUP = 128
CHUNK = 64
LAGS = (320, 160)
RAMP = (32, 32, 64)
WIDE = 512


def split(x):
    high = x.astype(jnp.bfloat16)
    return high, (x - high.astype(jnp.float32)).astype(jnp.bfloat16)


def product(left, right_high, right_low, right_dim):
    dims = (((1,), (right_dim,)), ((), ()))
    rows = left.shape[0]
    high, low = split(left)
    both = lax.dot_general(
        jnp.concatenate([high, low], axis=0), right_high, dims, preferred_element_type=jnp.float32
    )
    rest = lax.dot_general(high, right_low, dims, preferred_element_type=jnp.float32)
    return both[:rows] + (both[rows:] + rest)


def chunks_of(rhs):
    body = rhs - 2 * sum(RAMP)
    sizes = list(RAMP) + [CHUNK] * (body // CHUNK)
    if body % CHUNK:
        sizes.append(body % CHUNK)
    sizes += list(RAMP)[::-1]
    starts = [sum(sizes[:at]) for at in range(len(sizes))]
    return list(zip(starts, sizes))


def order_of(chunks, levels):
    steps = []
    for at, (start, size) in enumerate(chunks):
        for level in range(levels):
            lag = LAGS[0] * ((level + 1) // 2) + LAGS[1] * (level // 2)
            steps.append((start + lag, -level, at, level))
    return [(at, -low) for _, low, at, _ in sorted(steps)]


def partner(level, levels):
    axis = "row" if level % 2 == 0 else "col"
    span = lax.axis_size(axis) >> (1 + level // 2)
    me = lax.axis_index(axis)
    return {axis: me + span - 2 * span * ((me // span) % 2)}


def kernel(
    src, leaf, tra, res,
    src_v, leaf_v, tra_v, coeff, other, t_high, t_low,
    in_sem, tra_sem, out_sem, send_sem, recv_sem,
):
    levels, rank = tra.shape[0], leaf.shape[1]
    rhs = src.shape[1]
    groups = rhs // GROUP
    chunks = chunks_of(rhs)
    partners = [partner(level, levels) for level in range(levels)]

    barrier = pltpu.get_barrier_semaphore()
    for who in partners:
        pl.semaphore_signal(barrier, inc=1, device_id=who, device_id_type=pl.DeviceIdType.MESH)

    load_leaf = pltpu.make_async_copy(leaf, leaf_v, in_sem.at[groups])
    load_leaf.start()
    load_src = []
    for g in range(groups):
        cols = pl.ds(g * GROUP, GROUP)
        load_src.append(pltpu.make_async_copy(src.at[:, cols], src_v.at[:, cols], in_sem.at[g]))
        load_src[-1].start()
    load_tra = [pltpu.make_async_copy(tra.at[k], tra_v.at[k], tra_sem.at[k]) for k in range(levels)]
    for copy in load_tra:
        copy.start()

    copies = {}

    def send(at, level):
        rows = pl.ds(*chunks[at])
        copy = pltpu.make_async_remote_copy(
            src_ref=coeff.at[level, rows],
            dst_ref=other.at[level, rows],
            send_sem=send_sem.at[level, at],
            recv_sem=recv_sem.at[level, at],
            device_id=partners[level],
            device_id_type=pl.DeviceIdType.MESH,
        )
        copy.start()
        copies[at, level] = copy

    load_leaf.wait()
    l_high, l_low = split(leaf_v[...])
    for g in range(groups):
        load_src[g].wait()
        turned = src_v[:, g * GROUP:(g + 1) * GROUP].T
        coeff[0, pl.ds(g * GROUP, GROUP), :] = product(turned, l_high, l_low, 0)
        if g == 0:
            pl.semaphore_wait(barrier, levels)
        for at, (start, size) in enumerate(chunks):
            if g * GROUP < start + size <= (g + 1) * GROUP:
                send(at, 0)
    def prepare(k):
        load_tra[k].wait()
        high, low = split(tra_v[k].T)
        t_high[k] = high
        t_low[k] = low

    def mix(k, left, half):
        part = slice(half * rank, (half + 1) * rank)
        return product(left, t_high[k, part, :], t_low[k, part, :], 0)

    prepared = 0

    stores = []
    for at, level in order_of(chunks, levels):
        rows = pl.ds(*chunks[at])
        if level == prepared:
            prepare(level)
            prepared += 1
        own = mix(level, coeff[level, rows, :], 0)
        copies[at, level].wait_recv()
        fresh = own + mix(level, other[level, rows, :], 1)
        coeff[level + 1, rows, :] = fresh
        if level + 1 < levels:
            send(at, level + 1)
            continue
        stores.append(pltpu.make_async_copy(coeff.at[levels, rows], res.at[rows], out_sem.at[at]))
        stores[-1].start()
    for copy in copies.values():
        copy.wait_send()
    for copy in stores:
        copy.wait()


def expand(last, outb, res):
    last_high, last_low = split(last[...])
    res[...] = product(outb[...], last_high, last_low, 1)


def body(sources, leaf_basis, transfers, out_basis):
    src, leaf, tra, outb = sources[0, 0], leaf_basis[0, 0], transfers[0, 0], out_basis[0, 0]
    size, rhs = src.shape
    rank = leaf.shape[1]
    count = len(chunks_of(rhs))
    levels = tra.shape[0]
    f32 = jnp.float32
    any_space = pl.BlockSpec(memory_space=pl.ANY)
    hbm = pl.BlockSpec(memory_space=pltpu.HBM)
    last = pl.pallas_call(
        kernel,
        out_shape=jax.ShapeDtypeStruct((rhs, rank), f32),
        in_specs=[hbm] * 3,
        out_specs=any_space,
        scratch_shapes=[
            pltpu.VMEM((size, rhs), f32),
            pltpu.VMEM((size, rank), f32),
            pltpu.VMEM(tra.shape, f32),
            pltpu.VMEM((levels + 1, rhs, rank), f32),
            pltpu.VMEM((levels, rhs, rank), f32),
            pltpu.VMEM((levels, 2 * rank, rank), jnp.bfloat16),
            pltpu.VMEM((levels, 2 * rank, rank), jnp.bfloat16),
            pltpu.SemaphoreType.DMA((rhs // GROUP + 1,)),
            pltpu.SemaphoreType.DMA((levels,)),
            pltpu.SemaphoreType.DMA((count,)),
            pltpu.SemaphoreType.DMA((levels, count)),
            pltpu.SemaphoreType.DMA((levels, count)),
        ],
        compiler_params=pltpu.CompilerParams(collective_id=0, has_side_effects=True),
    )(src, leaf, tra)
    wide = min(WIDE, rhs)
    result = pl.pallas_call(
        expand,
        grid=(rhs // wide,),
        out_shape=jax.ShapeDtypeStruct((size, rhs), f32),
        in_specs=[
            pl.BlockSpec((wide, rank), lambda i: (i, 0)),
            pl.BlockSpec((size, rank), lambda i: (0, 0)),
        ],
        out_specs=pl.BlockSpec((size, wide), lambda i: (0, i)),
    )(last, outb)
    return result[None, None]


def solution(mesh):
    in_specs = (
        P("row", "col", None, None),
        P("row", "col", None, None),
        P("row", "col", None, None, None),
        P("row", "col", None, None),
    )
    out_specs = P("row", "col", None, None)
    return jax.shard_map(body, mesh=mesh, in_specs=in_specs, out_specs=out_specs, check_vma=False)
```
